1024 devices in a mesh: group: 32 (over x, y_hi, core), resp: 32 (over z, y_lo).
Axes of the slice: x: 4, y: 8 (y_hi: 4, y_lo: 2; y = y_hi * 2 + y_lo), z: 16, core: 2. Of those that a mesh axis runs over, the one named last changes fastest.
Arguments:
- prompt_hidden: bfloat16 [32, 256, 4096], P('group', 'resp'), may hold values from -6 to 6
- kv_weight: bfloat16 [2048, 4096], P('resp'), may hold values from -0.09375 to 0.09375
- queries: bfloat16 [32, 4096, 4096], P('group', 'resp'), may hold values from -150 to 150
- resp_keys: bfloat16 [32, 4096, 1024], P('group', 'resp'), may hold values from -5 to 5
- resp_values: bfloat16 [32, 4096, 1024], P('group', 'resp'), may hold values from -6 to 6
- upstream: bfloat16 [32, 4096, 4096], P('group', 'resp'), may hold values from -6 to 6
- signs: int32 [32, 4096], P('group', 'resp'), may hold values from -1 to 1
- lengths: int32 [32, 32], P('group', 'resp'), may hold values from 64 to 128
Outputs:
- grad_keys: bfloat16 [32, 4096, 1024], P('group', 'resp')
- grad_values: bfloat16 [32, 4096, 1024], P('group', 'resp')
- grad_weight: float32 [2048, 4096], P('resp', 'group')
The draws below stay inside these ranges and needn't reach their ends.
All inputs are finite; a program needn't handle non-finite values.
Results may differ from the reference program's by a relative error of at most 0.025.
Values may be sent and summed in bfloat16 or wider, within the bound.
A program may use at most 32 MiB of HBM per device.

```python
import math
import jax
import jax.numpy as jnp
from jax import lax

D = 4096
HEADS = 32
KV_HEADS = 8
HEAD = 128
R_DEV = 128
QW = 4096
KVW = 1024
RESPONSES = 32
GROUPS = 32
PROMPT = 256
TOK_RESP = 4096


def shared_draw(key):
    base_key = jax.random.fold_in(key, 7)
    key_width = KV_HEADS * HEAD
    key_rows = jnp.clip(jax.random.normal(jax.random.fold_in(base_key, 1), (GROUPS, TOK_RESP, key_width), jnp.float32), -5.0, 5.0)
    query_rows = jnp.clip(jax.random.normal(jax.random.fold_in(base_key, 2), (GROUPS, TOK_RESP, HEADS * HEAD), jnp.float32), -5.0, 5.0)
    return (key_rows, query_rows)


def draw_resp_keys(key, part):
    return shared_draw(key)[0].astype(jnp.bfloat16)


def draw_queries(key, part):
    return shared_draw(key)[1].astype(jnp.bfloat16)


def place_ends(result, rng, smallest, high):
    longest = result.shape.index(max(result.shape))
    spots = []
    for shift in (0, 1):
        where = [jax.random.randint(jax.random.fold_in(rng, axis), (), 0, length) for axis, length in enumerate(result.shape)]
        where[longest] = (where[longest] + shift) % result.shape[longest]
        spots.append(tuple(where))
    return result.at[spots[0]].set(smallest).at[spots[1]].set(high)


def strengthened(entries, key, source, target, blocks, factor):
    def block_of(axis_at):
        return (jnp.arange(entries.shape[axis_at]) // (entries.shape[axis_at] // blocks)).reshape((-1,) + (1,) * (entries.ndim - 1 - axis_at))

    near = jax.random.permutation(key, blocks)[block_of(target)]
    far = (block_of(target) + blocks // 2) % blocks
    return jnp.where((block_of(source) == near) | (block_of(source) == far), factor * entries, entries)


def block_levels(key, extent, cuts, least, high):
    def one(dim, parts):
        draws = jax.random.uniform(jax.random.fold_in(jax.random.fold_in(key, 6), dim), (parts,), jnp.float32, least / len(cuts), high / len(cuts))
        return jnp.repeat(jnp.exp(draws), extent[dim] // parts).reshape((-1,) + (1,) * (len(extent) - dim - 1))

    loudness = one(*cuts[0])
    for cut in cuts[1:]:
        loudness = loudness * one(*cut)
    return loudness


def normal_values(key, extent, scale, reach, cuts=(), kind=jnp.bfloat16):
    result = scale * jax.random.normal(key, extent, jnp.float32)
    if cuts:
        result = result * block_levels(key, extent, cuts, -0.22, 0.18)
    return jnp.clip(result, -reach, reach).astype(kind)


def gaussian_with(rng, extent, deviation, limit, cuts, heavy, held_as=jnp.bfloat16):
    values = deviation * jax.random.normal(rng, extent, jnp.float32)
    if cuts:
        values = values * block_levels(rng, extent, cuts, -0.22, 0.18)
    return jnp.clip(strengthened(values, jax.random.fold_in(rng, 3), *heavy), -limit, limit).astype(held_as)


def setup_inputs(seed: int = 0) -> dict:
    streams_of = jax.random.split(jax.random.key(seed), 9)
    return {
        "prompt_hidden": gaussian_with(streams_of[0], (GROUPS, PROMPT, D), 1.0, 6.0, ((0, 32), (1, 32)), (0, 2, 32, 2.75)),
        "kv_weight": normal_values(streams_of[1], (2 * KVW, D), D ** -0.5, 0.09375, ((0, 32),)),
        "queries": draw_queries(jax.random.fold_in(streams_of[8], 71), 0),
        "resp_keys": draw_resp_keys(jax.random.fold_in(streams_of[8], 71), 0),
        "resp_values": normal_values(streams_of[4], (GROUPS, TOK_RESP, KVW), 1.0, 6.0, ((0, 32), (1, 32))),
        "upstream": gaussian_with(streams_of[5], (GROUPS, TOK_RESP, QW), 1.0, 6.0, ((0, 32), (1, 32)), (1, 2, 32, 2.75)),
        "signs": place_ends(jax.random.randint(streams_of[6], (GROUPS, TOK_RESP), -1, 2), jax.random.fold_in(streams_of[6], 1), -1, 1).astype(jnp.int32),
        "lengths": place_ends(jax.random.randint(streams_of[7], (GROUPS, RESPONSES), R_DEV // 2, R_DEV + 1), jax.random.fold_in(streams_of[7], 1), R_DEV // 2, R_DEV).astype(jnp.int32),
    }


def attend(queries, cotangent, own_keys, own_values, prompt_keys, prompt_values):
    seq_len = queries.shape[0]
    per_head = HEADS // KV_HEADS
    scaling = 1.0 / math.sqrt(HEAD)
    query_full = queries.astype(jnp.float32).reshape(seq_len, KV_HEADS, per_head, HEAD)
    cotangent_full = cotangent.astype(jnp.float32).reshape(seq_len, KV_HEADS, per_head, HEAD)
    key_own = own_keys.astype(jnp.float32).reshape(seq_len, KV_HEADS, HEAD)
    value_own = own_values.astype(jnp.float32).reshape(seq_len, KV_HEADS, HEAD)
    key_prompt = prompt_keys.astype(jnp.float32).reshape(-1, KV_HEADS, HEAD)
    value_prompt = prompt_values.astype(jnp.float32).reshape(-1, KV_HEADS, HEAD)
    prompt_scores = jnp.einsum('rgqd,pgd->gqrp', query_full, key_prompt) * scaling
    own_scores = jnp.einsum('rgqd,sgd->gqrs', query_full, key_own) * scaling
    rows_index = jnp.arange(seq_len, dtype=jnp.int32)
    causal = rows_index[:, None] >= rows_index[None, :]
    own_scores = jnp.where(causal, own_scores, -jnp.inf)
    highest = jnp.maximum(lax.optimization_barrier(jnp.max(prompt_scores, axis=-1)), lax.optimization_barrier(jnp.max(own_scores, axis=-1)))[..., None]
    prompt_exp = jnp.exp(prompt_scores - highest)
    own_exp = jnp.exp(own_scores - highest)
    denominator = (lax.optimization_barrier(jnp.sum(prompt_exp, axis=-1)) + lax.optimization_barrier(jnp.sum(own_exp, axis=-1)))[..., None]
    prompt_probs = prompt_exp / denominator
    own_probs = own_exp / denominator
    prompt_half = prompt_probs.astype(jnp.bfloat16).astype(jnp.float32)
    own_half = own_probs.astype(jnp.bfloat16).astype(jnp.float32)
    mixed = jnp.einsum('gqrp,pgd->gqrd', prompt_half, value_prompt) + jnp.einsum('gqrs,sgd->gqrd', own_half, value_own)
    delta = jnp.einsum('gqrd,rgqd->gqr', mixed, cotangent_full)[..., None]
    prompt_dots = jnp.einsum('rgqd,pgd->gqrp', cotangent_full, value_prompt)
    own_dots = jnp.einsum('rgqd,sgd->gqrs', cotangent_full, value_own)
    prompt_sgrad = (prompt_probs * (prompt_dots - delta)).astype(jnp.bfloat16).astype(jnp.float32)
    own_sgrad = (own_probs * (own_dots - delta)).astype(jnp.bfloat16).astype(jnp.float32)
    key_terms = jnp.einsum('gqrp,rgqd->pgd', prompt_sgrad, query_full) * scaling
    value_terms = jnp.einsum('gqrp,rgqd->pgd', prompt_half, cotangent_full)
    key_grads = jnp.einsum('gqrs,rgqd->sgd', own_sgrad, query_full) * scaling
    value_grads = jnp.einsum('gqrs,rgqd->sgd', own_half, cotangent_full)
    key_width = KV_HEADS * HEAD
    return (key_terms.reshape(-1, key_width), value_terms.reshape(-1, key_width), key_grads.reshape(seq_len, key_width).astype(jnp.bfloat16), value_grads.reshape(seq_len, key_width).astype(jnp.bfloat16))

def reference(prompt_hidden, kv_weight, queries, resp_keys, resp_values, upstream, signs, lengths):
    key_width = KV_HEADS * HEAD
    positions = jnp.arange(R_DEV, dtype=jnp.int32)

    def per_group(carry_sum, inputs):
        hidden_rows, group_queries, group_keys, group_values, group_upstream, group_signs, group_lengths = inputs
        projected = jnp.dot(hidden_rows, kv_weight.T, preferred_element_type=jnp.float32).astype(jnp.bfloat16)
        prompt_keys = projected[:, :key_width]
        prompt_values = projected[:, key_width:]

        def per_response(pieces):
            resp_query, resp_key, resp_value, resp_upstream, resp_sign, resp_length = pieces
            live_rows = (positions < resp_length).astype(jnp.int32)
            weights = (resp_sign * live_rows).astype(jnp.bfloat16)
            cotangent = resp_upstream * weights[:, None]
            return attend(resp_query, cotangent, resp_key, resp_value, prompt_keys, prompt_values)
        key_terms, value_terms, key_grads, value_grads = lax.map(per_response, (group_queries.reshape(RESPONSES, R_DEV, -1), group_keys.reshape(RESPONSES, R_DEV, -1), group_values.reshape(RESPONSES, R_DEV, -1), group_upstream.reshape(RESPONSES, R_DEV, -1), group_signs.reshape(RESPONSES, R_DEV), group_lengths))
        prompt_grad = jnp.concatenate([lax.optimization_barrier(jnp.sum(key_terms, axis=0)), lax.optimization_barrier(jnp.sum(value_terms, axis=0))], axis=1)
        grad_half = prompt_grad.astype(jnp.bfloat16)
        weight_terms = jnp.dot(grad_half.T, hidden_rows, preferred_element_type=jnp.float32)
        return (carry_sum + weight_terms, (key_grads.reshape(TOK_RESP, key_width), value_grads.reshape(TOK_RESP, key_width)))
    initial = jnp.zeros((2 * key_width, D), jnp.float32)
    grad_weight, outputs = lax.scan(per_group, initial, (prompt_hidden, queries, resp_keys, resp_values, upstream, signs, lengths))
    return (outputs[0], outputs[1], grad_weight)
```

```python
import functools
import math

import jax
import jax.numpy as jnp
from jax import lax
from jax.experimental import pallas as pl
from jax.experimental.pallas import tpu as pltpu
from jax.sharding import PartitionSpec as P

MESH = pl.DeviceIdType.MESH
F32 = jnp.float32
BF16 = jnp.bfloat16
KV_HEADS = 8
PER_HEAD = 4
HEAD = 128
D = 4096
SEQ = 128
PROMPT = 256
NZ = 16
NCHIP = 16
NCH = 4
NOTHER = 2
CW = D // NCH
RIGHT, LEFT = 0, 1


def kernel(
    hid_in, w_in, q_in, rk_in, rv_in, up_in, signs_in, len_in,
    gk_out, gv_out, gw_out,
    hid, hid2, wbuf, q, rk, rv, cot, qt, ct, kt_own, vt_own,
    kvb, ph, ds, terms, yrecv, esend, erecv, own32, dsend, drecv, gsend, grecv,
    load_sem, a_send, a_recv, ay_send, ay_recv, c_send, c_recv, cy_send, cy_recv,
    e_send, e_recv, ey_send, ey_recv, d_send, d_recv, g_send, g_recv,
):
    g = lax.axis_index("group")
    r = lax.axis_index("resp")
    z, y = r // 2, lax.rem(r, 2)
    chip, core = g // 2, lax.rem(g, 2)

    def zmod(value):
        return lax.rem(value + 2 * NZ, NZ)

    up_z = {"resp": zmod(z + 1) * 2 + y}
    down_z = {"resp": zmod(z - 1) * 2 + y}
    partner = {"resp": z * 2 + 1 - y}
    twin = {"group": chip * 2 + 1 - core}
    to = (up_z, down_z)
    sign = (-1, 1)

    def peer(i):
        return lax.rem(chip + i, NCHIP)

    loads = [
        pltpu.make_async_copy(hid_in, hid.at[y, z], load_sem.at[0]),
        pltpu.make_async_copy(w_in, wbuf, load_sem.at[1]),
        pltpu.make_async_copy(q_in, q, load_sem.at[2]),
        pltpu.make_async_copy(up_in, cot, load_sem.at[3]),
        pltpu.make_async_copy(rk_in, rk, load_sem.at[4]),
        pltpu.make_async_copy(rv_in, rv, load_sem.at[5]),
    ]
    for load in loads:
        load.start()

    barrier = pltpu.get_barrier_semaphore()
    for target in (up_z, down_z, partner, twin):
        pl.semaphore_signal(barrier, inc=1, device_id=target, device_id_type=MESH)

    def greet(i, carry):
        pl.semaphore_signal(
            barrier, inc=1, device_id={"group": peer(i) * 2 + core}, device_id_type=MESH
        )
        return carry

    lax.fori_loop(1, NCHIP, greet, 0)
    pl.semaphore_wait(barrier, NCHIP - 1 + 4)
    loads[0].wait()

    def hid_piece(col, zz, c):
        return hid.at[col, zz, :, pl.ds(c * CW, CW)]

    def a_copy(d, s, slot, col, zz, c):
        return pltpu.make_async_remote_copy(
            src_ref=hid_piece(col, zz, c), dst_ref=hid_piece(col, zz, c),
            send_sem=a_send.at[d, s, slot], recv_sem=a_recv.at[d, s, slot],
            device_id=to[d], device_id_type=MESH,
        )

    def ay_copy(col, zz, c):
        return pltpu.make_async_remote_copy(
            src_ref=hid_piece(col, zz, c), dst_ref=hid_piece(col, zz, c),
            send_sem=ay_send.at[zz, c], recv_sem=ay_recv.at[zz, c],
            device_id=partner, device_id_type=MESH,
        )

    slots = [(0, c) for c in range(NCH)] + [(1, c) for c in range(NOTHER)]

    def column(kind):
        return y if kind == 0 else 1 - y

    def carried(d, slot, s_last):
        kind, c = slots[slot]
        if not s_last:
            return True
        half = (NCH if kind == 0 else NOTHER) // 2
        return (c < half) == (d == RIGHT)

    for c in range(NCH):
        ay_copy(y, z, c).start()
    for slot, (kind, c) in enumerate(slots):
        for d in (RIGHT, LEFT):
            if kind == 1 and d == RIGHT:
                ay_copy(1 - y, z, c).wait_recv()
            a_copy(d, 0, slot, column(kind), z, c).start()

    def a_step(s, last):
        for slot, (kind, c) in enumerate(slots):
            for d in (RIGHT, LEFT):
                zz = zmod(z + sign[d] * s)
                a_copy(d, s - 1, slot, column(kind), zz, c).wait_recv()
                if carried(d, slot, last):
                    a_copy(d, s, slot, column(kind), zz, c).start()
                if kind == 0 and c >= NOTHER:
                    ay_copy(y, zz, c).start()

    def prepare(j):
        weights = jnp.where(
            lax.broadcasted_iota(jnp.int32, (1, SEQ), 1) < len_in[...], signs_in[...], 0
        ).astype(F32)
        weights = jnp.broadcast_to(weights, (SEQ, SEQ)).T.astype(BF16)
        for i in range(PER_HEAD):
            cols = pl.ds(pl.multiple_of((j * PER_HEAD + i) * HEAD, HEAD), HEAD)
            qt[j, :, i * SEQ:(i + 1) * SEQ] = q[:, cols].T
            value = cot[:, cols] * weights
            cot[:, cols] = value
            ct[j, :, i * SEQ:(i + 1) * SEQ] = value.T
        cols = pl.ds(pl.multiple_of(j * HEAD, HEAD), HEAD)
        kt_own[j] = rk[:, cols].T
        vt_own[j] = rv[:, cols].T

    for load in loads[1:]:
        load.wait()
    prepare(0)

    def a_loop(s, carry):
        a_step(s, False)
        prepare(s)
        return carry

    lax.fori_loop(1, 7, a_loop, 0)
    a_step(7, True)
    prepare(7)
    far = zmod(z + 8)
    for slot, (kind, c) in enumerate(slots):
        d = RIGHT if carried(RIGHT, slot, True) else LEFT
        a_copy(d, 7, slot, column(kind), far, c).wait_recv()
        if kind == 0 and c >= NOTHER:
            ay_copy(y, far, c).start()
    for c in range(NOTHER, NCH):
        ay_copy(1 - y, z, c).wait_recv()

    def ay_wait(i, carry):
        for c in range(NOTHER, NCH):
            ay_copy(1 - y, zmod(z + i), c).wait_recv()
        return carry

    lax.fori_loop(1, NZ, ay_wait, 0)

    kw = 512
    total = jnp.zeros((64, PROMPT), F32)

    def project(i, total):
        cols = pl.ds(pl.multiple_of(i * kw, kw), kw)
        rows = hid[:, :, :, cols].astype(F32).reshape(PROMPT, kw).astype(BF16)
        hid2[:, cols] = rows
        return total + lax.dot_general(
            wbuf[:, cols], rows, (((1,), (1,)), ((), ())), preferred_element_type=F32
        )

    total = lax.fori_loop(0, D // kw, project, total)
    kvb[z, y] = total.astype(BF16)

    def kv_piece(zz, col, c):
        return kvb.at[zz, col, pl.ds(c * 32, 32), :]

    def c_copy(d, s, c, zz):
        return pltpu.make_async_remote_copy(
            src_ref=kv_piece(zz, y, c), dst_ref=kv_piece(zz, y, c),
            send_sem=c_send.at[d, s, c], recv_sem=c_recv.at[d, s, c],
            device_id=to[d], device_id_type=MESH,
        )

    def cy_copy(zz, col, c):
        return pltpu.make_async_remote_copy(
            src_ref=kv_piece(zz, col, c), dst_ref=kv_piece(zz, col, c),
            send_sem=cy_send.at[zz, c], recv_sem=cy_recv.at[zz, c],
            device_id=partner, device_id_type=MESH,
        )

    for c in range(2):
        for d in (RIGHT, LEFT):
            c_copy(d, 0, c, z).start()
        cy_copy(z, y, c).start()

    def c_step(s, last):
        for c in range(2):
            for d in (RIGHT, LEFT):
                zz = zmod(z + sign[d] * s)
                c_copy(d, s - 1, c, zz).wait_recv()
                if not last or c == d:
                    c_copy(d, s, c, zz).start()
                cy_copy(zz, y, c).start()

    def c_loop(s, carry):
        c_step(s, False)
        return carry

    lax.fori_loop(1, 7, c_loop, 0)
    c_step(7, True)
    for c in range(2):
        c_copy(c, 7, c, far).wait_recv()
        cy_copy(far, y, c).start()

    def cy_wait(i, carry):
        for c in range(2):
            cy_copy(zmod(z + i), 1 - y, c).wait_recv()
        return carry

    lax.fori_loop(0, NZ, cy_wait, 0)

    scaling = 1.0 / math.sqrt(HEAD)
    factor = scaling * math.log2(math.e)

    def attend(j, carry):
        keys = jnp.concatenate([kvb[j].reshape(HEAD, PROMPT), kt_own[j]], axis=1)
        values = jnp.concatenate([kvb[j + 8].reshape(HEAD, PROMPT), vt_own[j]], axis=1)
        shape = (SEQ, PROMPT + SEQ)
        at = lax.broadcasted_iota(jnp.int32, shape, 0)
        key_at = lax.broadcasted_iota(jnp.int32, shape, 1) - PROMPT
        seen = key_at <= at
        for i in range(PER_HEAD):
            cols = pl.ds(pl.multiple_of((j * PER_HEAD + i) * HEAD, HEAD), HEAD)
            rows = slice(i * SEQ, (i + 1) * SEQ)
            scores = jnp.dot(q[:, cols], keys, preferred_element_type=F32)
            scores = jnp.where(seen, scores, -jnp.inf)
            highest = jnp.max(scores, axis=1, keepdims=True)
            weight = jnp.exp2((scores - highest) * factor)
            probs = weight * (1.0 / jnp.sum(weight, axis=1, keepdims=True))
            half = probs.astype(BF16)
            ph[rows, :] = half
            dots = jnp.dot(cot[:, cols], values, preferred_element_type=F32)
            delta = jnp.sum(half.astype(F32) * dots, axis=1, keepdims=True)
            ds[rows, :] = (probs * (dots - delta)).astype(BF16)
        key_grad = jnp.dot(qt[j], ds[...], preferred_element_type=F32) * scaling
        value_grad = jnp.dot(ct[j], ph[...], preferred_element_type=F32)
        terms[j] = key_grad[:, :PROMPT].astype(BF16).reshape(2, 64, PROMPT)
        terms[j + 8] = value_grad[:, :PROMPT].astype(BF16).reshape(2, 64, PROMPT)
        cols = pl.ds(pl.multiple_of(j * HEAD, HEAD), HEAD)
        gk_out[:, cols] = key_grad[:, PROMPT:].T.astype(BF16)
        gv_out[:, cols] = value_grad[:, PROMPT:].T.astype(BF16)
        return carry

    lax.fori_loop(0, KV_HEADS, attend, 0)

    def ey_copy(zz, col):
        return pltpu.make_async_remote_copy(
            src_ref=terms.at[zz, col], dst_ref=yrecv.at[zz],
            send_sem=ey_send.at[zz], recv_sem=ey_recv.at[zz],
            device_id=partner, device_id_type=MESH,
        )

    def e_copy(d, s, c):
        part = pl.ds(c * 32, 32)
        return pltpu.make_async_remote_copy(
            src_ref=esend.at[d, s, part, :], dst_ref=erecv.at[d, s, part, :],
            send_sem=e_send.at[d, s, c], recv_sem=e_recv.at[d, s, c],
            device_id=to[d], device_id_type=MESH,
        )

    ey_copy(far, 1 - y).start()

    def ey_start(i, carry):
        ey_copy(zmod(z + 8 - i), 1 - y).start()
        ey_copy(zmod(z + 8 + i), 1 - y).start()
        return carry

    lax.fori_loop(1, 8, ey_start, 0)
    ey_copy(z, 1 - y).start()

    def pair_sum(zz, c):
        part = pl.ds(c * 32, 32)
        return terms[zz, y, part, :].astype(F32) + yrecv[zz, part, :].astype(F32)

    ey_copy(far, y).wait_recv()
    for d in (RIGHT, LEFT):
        esend[d, 0, pl.ds(d * 32, 32), :] = pair_sum(far, d).astype(BF16)
        e_copy(d, 0, d).start()

    def e_step(s, first):
        for d in (RIGHT, LEFT):
            ey_copy(zmod(z + sign[d] * (s - 8)), y).wait_recv()
        for c in range(2):
            part = pl.ds(c * 32, 32)
            for d in (RIGHT, LEFT):
                value = pair_sum(zmod(z + sign[d] * (s - 8)), c)
                if not first or c == d:
                    e_copy(d, s - 1, c).wait_recv()
                    value = value + erecv[d, s - 1, part, :].astype(F32)
                esend[d, s, part, :] = value.astype(BF16)
                e_copy(d, s, c).start()

    e_step(1, True)

    def e_loop(s, carry):
        e_step(s, False)
        return carry

    lax.fori_loop(2, 8, e_loop, 0)
    ey_copy(z, y).wait_recv()
    halves = []
    for c in range(2):
        part = pl.ds(c * 32, 32)
        value = pair_sum(z, c)
        for d in (RIGHT, LEFT):
            e_copy(d, 7, c).wait_recv()
            value = value + erecv[d, 7, part, :].astype(F32)
        halves.append(value.astype(BF16))
    prompt_grad = jnp.concatenate(halves, axis=0)

    def d_copy(b):
        part = pl.ds(b * 4, 4)
        return pltpu.make_async_remote_copy(
            src_ref=dsend.at[part], dst_ref=drecv.at[part],
            send_sem=d_send.at[b], recv_sem=d_recv.at[b],
            device_id=twin, device_id_type=MESH,
        )

    def g_copy(i):
        return pltpu.make_async_remote_copy(
            src_ref=gsend.at[i], dst_ref=grecv.at[i],
            send_sem=g_send.at[i], recv_sem=g_recv.at[i],
            device_id={"group": peer(i) * 2 + core}, device_id_type=MESH,
        )

    def weigh(i, carry):
        k = peer(i)
        cols = pl.ds(pl.multiple_of(k * 256, 256), 256)
        block = jnp.dot(prompt_grad, hid2[:, cols], preferred_element_type=F32)
        low, high = block[:, :128], block[:, 128:]
        own32[i] = jnp.where(core == 0, low, high)
        dsend[i] = jnp.where(core == 0, high, low).astype(BF16)
        return carry

    for b in range(4):
        lax.fori_loop(4 * b, 4 * b + 4, weigh, 0)
        d_copy(b).start()

    def send_out(i, carry):
        gsend[i] = (own32[i] + drecv[i].astype(F32)).astype(BF16)
        g_copy(i).start()
        return carry

    d_copy(0).wait_recv()
    result = own32[0] + drecv[0].astype(F32)
    lax.fori_loop(1, 4, send_out, 0)
    for b in range(1, 4):
        d_copy(b).wait_recv()
        lax.fori_loop(4 * b, 4 * b + 4, send_out, 0)

    for slot, (kind, c) in enumerate(slots):
        for d in (RIGHT, LEFT):
            def a_sent(s, carry, d=d, slot=slot, kind=kind, c=c):
                a_copy(d, s, slot, column(kind), z, c).wait_send()
                return carry

            lax.fori_loop(0, 8 if carried(d, slot, True) else 7, a_sent, 0)
    for c in range(NCH):
        ay_copy(y, z, c).wait_send()

    def sent(i, carry):
        zz = zmod(z + i)
        for c in range(NOTHER, NCH):
            ay_copy(y, zz, c).wait_send()
        return carry

    lax.fori_loop(1, NZ, sent, 0)

    def sent_each(i, carry):
        for c in range(2):
            cy_copy(i, y, c).wait_send()
        ey_copy(i, 1 - y).wait_send()
        return carry

    lax.fori_loop(0, NZ, sent_each, 0)
    for c in range(2):
        for d in (RIGHT, LEFT):
            def c_sent(s, carry, d=d, c=c):
                c_copy(d, s, c, z).wait_send()
                return carry

            def e_sent(s, carry, d=d, c=c):
                e_copy(d, s, c).wait_send()
                return carry

            lax.fori_loop(0, 8 if c == d else 7, c_sent, 0)
            lax.fori_loop(0 if c == d else 1, 8, e_sent, 0)
    for b in range(4):
        d_copy(b).wait_send()

    def g_sent(i, carry):
        g_copy(i).wait_send()
        return carry

    lax.fori_loop(1, NCHIP, g_sent, 0)

    def gather_sum(i, result):
        g_copy(i).wait_recv()
        return result + grecv[i].astype(F32)

    gw_out[...] = lax.fori_loop(1, NCHIP, gather_sum, result)


def per_device(prompt_hidden, kv_weight, queries, resp_keys, resp_values, upstream, signs, lengths):
    vmem = pl.BlockSpec(memory_space=pltpu.VMEM)
    anywhere = pl.BlockSpec(memory_space=pl.ANY)
    dma = pltpu.SemaphoreType.DMA
    nslot = NCH + NOTHER
    grad_keys, grad_values, grad_weight = pl.pallas_call(
        kernel,
        out_shape=(
            jax.ShapeDtypeStruct((SEQ, 1024), BF16),
            jax.ShapeDtypeStruct((SEQ, 1024), BF16),
            jax.ShapeDtypeStruct((64, 128), F32),
        ),
        in_specs=[anywhere] * 6 + [vmem] * 2,
        out_specs=(vmem, vmem, vmem),
        scratch_shapes=[
            pltpu.VMEM((2, NZ, 8, D), BF16),
            pltpu.VMEM((PROMPT, D), BF16),
            pltpu.VMEM((64, D), BF16),
            pltpu.VMEM((SEQ, D), BF16),
            pltpu.VMEM((SEQ, 1024), BF16),
            pltpu.VMEM((SEQ, 1024), BF16),
            pltpu.VMEM((SEQ, D), BF16),
            pltpu.VMEM((KV_HEADS, HEAD, 512), BF16),
            pltpu.VMEM((KV_HEADS, HEAD, 512), BF16),
            pltpu.VMEM((KV_HEADS, HEAD, SEQ), BF16),
            pltpu.VMEM((KV_HEADS, HEAD, SEQ), BF16),
            pltpu.VMEM((NZ, 2, 64, PROMPT), BF16),
            pltpu.VMEM((512, PROMPT + SEQ), BF16),
            pltpu.VMEM((512, PROMPT + SEQ), BF16),
            pltpu.VMEM((NZ, 2, 64, PROMPT), BF16),
            pltpu.VMEM((NZ, 64, PROMPT), BF16),
            pltpu.VMEM((2, 8, 64, PROMPT), BF16),
            pltpu.VMEM((2, 8, 64, PROMPT), BF16),
            pltpu.VMEM((NCHIP, 64, 128), F32),
            pltpu.VMEM((NCHIP, 64, 128), BF16),
            pltpu.VMEM((NCHIP, 64, 128), BF16),
            pltpu.VMEM((NCHIP, 64, 128), BF16),
            pltpu.VMEM((NCHIP, 64, 128), BF16),
            dma((6,)),
            dma((2, 8, nslot)), dma((2, 8, nslot)), dma((NZ, NCH)), dma((NZ, NCH)),
            dma((2, 8, 2)), dma((2, 8, 2)), dma((NZ, 2)), dma((NZ, 2)),
            dma((2, 8, 2)), dma((2, 8, 2)), dma((NZ,)), dma((NZ,)),
            dma((4,)), dma((4,)), dma((NCHIP,)), dma((NCHIP,)),
        ],
        compiler_params=pltpu.CompilerParams(
            collective_id=0, has_side_effects=True, vmem_limit_bytes=63 * 1024 * 1024
        ),
    )(
        prompt_hidden[0], kv_weight, queries[0], resp_keys[0], resp_values[0], upstream[0],
        signs, lengths,
    )
    return grad_keys[None], grad_values[None], grad_weight


def solution(mesh):
    rows = P("group", "resp", None)
    return jax.shard_map(
        per_device,
        mesh=mesh,
        in_specs=(rows, P("resp", None), rows, rows, rows, rows, P("group", "resp"), P("group", "resp")),
        out_specs=(rows, rows, P("resp", "group")),
        check_vma=False,
    )
```

```python
import functools
import math

import jax
import jax.numpy as jnp
from jax import lax
from jax.experimental import pallas as pl
from jax.experimental.pallas import tpu as pltpu
from jax.sharding import PartitionSpec as P

MESH = pl.DeviceIdType.MESH
F32 = jnp.float32
BF16 = jnp.bfloat16
KV_HEADS = 8
PER_HEAD = 4
HEAD = 128
D = 4096
SEQ = 128
PROMPT = 256
NZ = 16
NCHIP = 16
NCH = 2
NOTHER = 0
CW = D // NCH
CHILDREN = {
    0: (4, -4, 1, -1), 4: (8, 6, 5, 3), -4: (8, -6, -5, -3),
    1: (2,), -1: (-2,), 6: (7,), -6: (-7,),
}
ARRIVALS = ((4, -4), (1, -1), (6, -6), (2, -2), (5, -5), (3, -3), (8,), (7, -7))
A_CHILDREN = {0: (2, -2, 1, -1), 2: (4, 3), -2: (-4, -3), 4: (6, 5), -4: (-6, -5), 6: (8, 7), -6: (8, -7)}
A_ARRIVALS = ((2, -2), (1, -1), (4, -4), (3, -3), (6, -6), (5, -5), (8,), (7, -7))
A_SENDS = tuple((o, child) for o, children in A_CHILDREN.items() for child in children)
MOVES = (1, -1, 2, -2, 4, -4)
SENDS = tuple((o, child) for o, children in CHILDREN.items() for child in children)
HEAD_ORDER = sum(k * 8**i for i, k in enumerate((4, 0, 1, 7, 5, 3, 2, 6)))


def takes(o, child, index, count):
    return child != 8 or (o > 0) == (index < (count + 1) // 2)


def kernel(
    hid_in, w_in, q_in, rk_in, rv_in, up_in, signs_in, len_in,
    gk_out, gv_out, gw_out,
    hid, hid2, wbuf, q, rk, rv, cot, qt, ct, kt_own, vt_own,
    kvb, ph, ds, terms, yrecv, esend, erecv, own32, dsend, drecv, gsend, grecv,
    load_sem, a_send, a_recv, ay_send, ay_recv, c_send, c_recv, cy_send, cy_recv,
    e_send, e_recv, ey_send, ey_recv, d_send, d_recv, g_send, g_recv,
):
    g = lax.axis_index("group")
    r = lax.axis_index("resp")
    z, y = r // 2, lax.rem(r, 2)
    chip, core = g // 2, lax.rem(g, 2)

    def zmod(value):
        return lax.rem(value + 2 * NZ, NZ)

    partner = {"resp": z * 2 + 1 - y}
    twin = {"group": chip * 2 + 1 - core}

    def along(step):
        return {"resp": zmod(z + step) * 2 + y}

    def peer(i):
        return lax.rem(chip + i, NCHIP)

    loads = [
        pltpu.make_async_copy(hid_in, hid.at[y, z], load_sem.at[0]),
        pltpu.make_async_copy(w_in, wbuf, load_sem.at[1]),
        pltpu.make_async_copy(q_in, q, load_sem.at[2]),
        pltpu.make_async_copy(up_in, cot, load_sem.at[3]),
        pltpu.make_async_copy(rk_in, rk, load_sem.at[4]),
        pltpu.make_async_copy(rv_in, rv, load_sem.at[5]),
    ]
    for load in loads:
        load.start()

    barrier = pltpu.get_barrier_semaphore()
    for target in (partner, twin, *map(along, MOVES)):
        pl.semaphore_signal(barrier, inc=1, device_id=target, device_id_type=MESH)

    def greet(i, carry):
        pl.semaphore_signal(
            barrier, inc=1, device_id={"group": peer(i) * 2 + core}, device_id_type=MESH
        )
        return carry

    lax.fori_loop(1, NCHIP, greet, 0)
    pl.semaphore_wait(barrier, NCHIP - 1 + 2 + len(MOVES))
    loads[0].wait()

    def hid_piece(col, zz, c):
        return hid.at[col, zz, :, pl.ds(c * CW, CW)]

    def a_copy(o, child, slot):
        kind, c = slots[slot]
        piece = hid_piece(column(kind), zmod(z - o), c)
        return pltpu.make_async_remote_copy(
            src_ref=piece, dst_ref=piece,
            send_sem=a_send.at[child % NZ, slot], recv_sem=a_recv.at[child % NZ, slot],
            device_id=along(child - o), device_id_type=MESH,
        )

    def a_arrived(o, slot):
        kind, c = slots[slot]
        piece = hid_piece(column(kind), zmod(z - o), c)
        pltpu.make_async_remote_copy(
            src_ref=piece, dst_ref=piece,
            send_sem=a_send.at[o % NZ, slot], recv_sem=a_recv.at[o % NZ, slot],
            device_id=partner, device_id_type=MESH,
        ).wait_recv()

    def ay_copy(col, zz, c):
        return pltpu.make_async_remote_copy(
            src_ref=hid_piece(col, zz, c), dst_ref=hid_piece(col, zz, c),
            send_sem=ay_send.at[zz, c], recv_sem=ay_recv.at[zz, c],
            device_id=partner, device_id_type=MESH,
        )

    slots = [(0, c) for c in range(NCH)] + [(1, c) for c in range(NOTHER)]

    def column(kind):
        return y if kind == 0 else 1 - y

    def a_takes(o, child, slot):
        kind, c = slots[slot]
        return takes(o, child, c, NCH if kind == 0 else NOTHER)

    def a_forward(o, slot, children):
        for child in children:
            if a_takes(o, child, slot):
                a_copy(o, child, slot).start()

    for at, children in enumerate((A_CHILDREN[0][:2], A_CHILDREN[0][2:])):
        for slot in range(NCH):
            a_forward(0, slot, children)
            if at == 0:
                ay_copy(y, z, slot).start()
    for slot in range(NCH, NCH + NOTHER):
        ay_copy(1 - y, z, slots[slot][1]).wait_recv()
        a_forward(0, slot, A_CHILDREN[0])

    def prepare(j):
        weights = jnp.where(
            lax.broadcasted_iota(jnp.int32, (1, SEQ), 1) < len_in[...], signs_in[...], 0
        ).astype(F32)
        weights = jnp.broadcast_to(weights, (SEQ, SEQ)).T.astype(BF16)
        for i in range(PER_HEAD):
            cols = pl.ds(pl.multiple_of((j * PER_HEAD + i) * HEAD, HEAD), HEAD)
            qt[j, :, i * SEQ:(i + 1) * SEQ] = q[:, cols].T
            value = cot[:, cols] * weights
            cot[:, cols] = value
            ct[j, :, i * SEQ:(i + 1) * SEQ] = value.T
        cols = pl.ds(pl.multiple_of(j * HEAD, HEAD), HEAD)
        kt_own[j] = rk[:, cols].T
        vt_own[j] = rv[:, cols].T

    for load in loads[1:]:
        load.wait()

    def prepare_loop(j, carry):
        prepare(j)
        return carry

    lax.fori_loop(0, KV_HEADS, prepare_loop, 0)
    for offsets in A_ARRIVALS:
        for slot, (kind, c) in enumerate(slots):
            for o in offsets:
                a_arrived(o, slot)
                a_forward(o, slot, A_CHILDREN.get(o, ()))
                if kind == 0 and c >= NOTHER:
                    ay_copy(y, zmod(z - o), c).start()
    for c in range(NOTHER, NCH):
        ay_copy(1 - y, z, c).wait_recv()

    def ay_wait(i, carry):
        for c in range(NOTHER, NCH):
            ay_copy(1 - y, zmod(z + i), c).wait_recv()
        return carry

    lax.fori_loop(1, NZ, ay_wait, 0)

    kw = 512
    total = jnp.zeros((64, PROMPT), F32)

    def project(i, total):
        cols = pl.ds(pl.multiple_of(i * kw, kw), kw)
        rows = hid[:, :, :, cols].astype(F32).reshape(PROMPT, kw).astype(BF16)
        hid2[:, cols] = rows
        return total + lax.dot_general(
            wbuf[:, cols], rows, (((1,), (1,)), ((), ())), preferred_element_type=F32
        )

    total = lax.fori_loop(0, D // kw, project, total)
    kvb[z, y] = total.astype(BF16)

    def kv_piece(zz, col, c):
        return kvb.at[zz, col, pl.ds(c * 32, 32), :]

    def c_copy(o, child, c):
        piece = kv_piece(zmod(z - o), y, c)
        return pltpu.make_async_remote_copy(
            src_ref=piece, dst_ref=piece,
            send_sem=c_send.at[child % NZ, c], recv_sem=c_recv.at[child % NZ, c],
            device_id=along(child - o), device_id_type=MESH,
        )

    def c_arrived(o, c):
        piece = kv_piece(zmod(z - o), y, c)
        pltpu.make_async_remote_copy(
            src_ref=piece, dst_ref=piece,
            send_sem=c_send.at[o % NZ, c], recv_sem=c_recv.at[o % NZ, c],
            device_id=partner, device_id_type=MESH,
        ).wait_recv()

    def c_forward(o, c, children):
        for child in children:
            if takes(o, child, c, 2):
                c_copy(o, child, c).start()

    def cy_copy(zz, col, c):
        return pltpu.make_async_remote_copy(
            src_ref=kv_piece(zz, col, c), dst_ref=kv_piece(zz, col, c),
            send_sem=cy_send.at[zz, c], recv_sem=cy_recv.at[zz, c],
            device_id=partner, device_id_type=MESH,
        )

    for children in ((4, -4), (1, -1)):
        for c in range(2):
            c_forward(0, c, children)
            if children[0] == 4:
                cy_copy(z, y, c).start()
    for offsets in ARRIVALS:
        for c in range(2):
            for o in offsets:
                c_arrived(o, c)
                c_forward(o, c, CHILDREN.get(o, ()))
                cy_copy(zmod(z - o), y, c).start()

    scaling = 1.0 / math.sqrt(HEAD)
    factor = scaling * math.log2(math.e)

    def ey_copy(zz, col):
        return pltpu.make_async_remote_copy(
            src_ref=terms.at[zz, col], dst_ref=yrecv.at[zz],
            send_sem=ey_send.at[zz], recv_sem=ey_recv.at[zz],
            device_id=partner, device_id_type=MESH,
        )

    def attend(step, order):
        j = lax.rem(z + order % 8, 8)
        for c in range(2):
            cy_copy(j, 1 - y, c).wait_recv()
            cy_copy(j + 8, 1 - y, c).wait_recv()
        keys = jnp.concatenate([kvb[j].reshape(HEAD, PROMPT), kt_own[j]], axis=1)
        values = jnp.concatenate([kvb[j + 8].reshape(HEAD, PROMPT), vt_own[j]], axis=1)
        shape = (SEQ, PROMPT + SEQ)
        at = lax.broadcasted_iota(jnp.int32, shape, 0)
        key_at = lax.broadcasted_iota(jnp.int32, shape, 1) - PROMPT
        seen = key_at <= at
        for i in range(PER_HEAD):
            cols = pl.ds(pl.multiple_of((j * PER_HEAD + i) * HEAD, HEAD), HEAD)
            rows = slice(i * SEQ, (i + 1) * SEQ)
            scores = jnp.dot(q[:, cols], keys, preferred_element_type=F32)
            scores = jnp.where(seen, scores, -jnp.inf)
            highest = jnp.max(scores, axis=1, keepdims=True)
            weight = jnp.exp2((scores - highest) * factor)
            probs = weight * (1.0 / jnp.sum(weight, axis=1, keepdims=True))
            half = probs.astype(BF16)
            ph[rows, :] = half
            dots = jnp.dot(cot[:, cols], values, preferred_element_type=F32)
            delta = jnp.sum(half.astype(F32) * dots, axis=1, keepdims=True)
            ds[rows, :] = (probs * (dots - delta)).astype(BF16)
        key_grad = jnp.dot(qt[j], ds[...], preferred_element_type=F32) * scaling
        value_grad = jnp.dot(ct[j], ph[...], preferred_element_type=F32)
        terms[j] = key_grad[:, :PROMPT].astype(BF16).reshape(2, 64, PROMPT)
        terms[j + 8] = value_grad[:, :PROMPT].astype(BF16).reshape(2, 64, PROMPT)
        ey_copy(j, 1 - y).start()
        ey_copy(j + 8, 1 - y).start()
        cols = pl.ds(pl.multiple_of(j * HEAD, HEAD), HEAD)
        gk_out[:, cols] = key_grad[:, PROMPT:].T.astype(BF16)
        gv_out[:, cols] = value_grad[:, PROMPT:].T.astype(BF16)
        return order // 8

    lax.fori_loop(0, KV_HEADS, attend, HEAD_ORDER)

    def e_copy(o, parent):
        part = pl.ds(0, 64) if o != 8 else pl.ds(0 if parent == 4 else 32, 32)
        return pltpu.make_async_remote_copy(
            src_ref=esend.at[o % NZ, part, :], dst_ref=erecv.at[o % NZ, part, :],
            send_sem=e_send.at[o % NZ, int(parent < 0)],
            recv_sem=e_recv.at[o % NZ, int(parent < 0)],
            device_id=along(parent - o), device_id_type=MESH,
        )

    def partial(o, c):
        zz = zmod(z - o)
        part = pl.ds(c * 32, 32)
        value = terms[zz, y, part, :].astype(F32) + yrecv[zz, part, :].astype(F32)
        for child in CHILDREN.get(o, ()):
            if child != 8 or (o > 0) == (c == 0):
                value = value + erecv[child % NZ, part, :].astype(F32)
        return value.astype(BF16)

    def collect(o):
        ey_copy(zmod(z - o), y).wait_recv()
        for child in CHILDREN.get(o, ()):
            e_copy(child, o).wait_recv()

    for o in (7, -7, 8, 5, -5, 3, -3, 2, -2, 6, -6, 1, -1, 4, -4):
        collect(o)
        for c in range(2):
            esend[o % NZ, pl.ds(c * 32, 32), :] = partial(o, c)
        for parent, children in CHILDREN.items():
            if o in children:
                e_copy(o, parent).start()
    collect(0)
    prompt_grad = jnp.concatenate([partial(0, c) for c in range(2)], axis=0)

    def d_copy(b):
        part = pl.ds(b * 4, 4)
        return pltpu.make_async_remote_copy(
            src_ref=dsend.at[part], dst_ref=drecv.at[part],
            send_sem=d_send.at[b], recv_sem=d_recv.at[b],
            device_id=twin, device_id_type=MESH,
        )

    def g_copy(i):
        return pltpu.make_async_remote_copy(
            src_ref=gsend.at[i], dst_ref=grecv.at[i],
            send_sem=g_send.at[i], recv_sem=g_recv.at[i],
            device_id={"group": peer(i) * 2 + core}, device_id_type=MESH,
        )

    def weigh(i, carry):
        k = peer(i)
        cols = pl.ds(pl.multiple_of(k * 256, 256), 256)
        block = jnp.dot(prompt_grad, hid2[:, cols], preferred_element_type=F32)
        low, high = block[:, :128], block[:, 128:]
        own32[i] = jnp.where(core == 0, low, high)
        dsend[i] = jnp.where(core == 0, high, low).astype(BF16)
        return carry

    for b in range(4):
        lax.fori_loop(4 * b, 4 * b + 4, weigh, 0)
        d_copy(b).start()

    def send_out(i, carry):
        gsend[i] = (own32[i] + drecv[i].astype(F32)).astype(BF16)
        g_copy(i).start()
        return carry

    d_copy(0).wait_recv()
    result = own32[0] + drecv[0].astype(F32)
    lax.fori_loop(1, 4, send_out, 0)
    for b in range(1, 4):
        d_copy(b).wait_recv()
        lax.fori_loop(4 * b, 4 * b + 4, send_out, 0)

    for o, child in A_SENDS:
        for slot in range(len(slots)):
            if a_takes(o, child, slot):
                a_copy(o, child, slot).wait_send()
    for c in range(NCH):
        ay_copy(y, z, c).wait_send()

    def sent(i, carry):
        zz = zmod(z + i)
        for c in range(NOTHER, NCH):
            ay_copy(y, zz, c).wait_send()
        return carry

    lax.fori_loop(1, NZ, sent, 0)

    def sent_each(i, carry):
        for c in range(2):
            cy_copy(i, y, c).wait_send()
        ey_copy(i, 1 - y).wait_send()
        return carry

    lax.fori_loop(0, NZ, sent_each, 0)
    for o, child in SENDS:
        for c in range(2):
            if takes(o, child, c, 2):
                c_copy(o, child, c).wait_send()
        e_copy(child, o).wait_send()
    for b in range(4):
        d_copy(b).wait_send()

    def g_sent(i, carry):
        g_copy(i).wait_send()
        return carry

    lax.fori_loop(1, NCHIP, g_sent, 0)

    def gather_sum(i, result):
        g_copy(i).wait_recv()
        return result + grecv[i].astype(F32)

    gw_out[...] = lax.fori_loop(1, NCHIP, gather_sum, result)


def per_device(prompt_hidden, kv_weight, queries, resp_keys, resp_values, upstream, signs, lengths):
    vmem = pl.BlockSpec(memory_space=pltpu.VMEM)
    anywhere = pl.BlockSpec(memory_space=pl.ANY)
    dma = pltpu.SemaphoreType.DMA
    nslot = NCH + NOTHER
    grad_keys, grad_values, grad_weight = pl.pallas_call(
        kernel,
        out_shape=(
            jax.ShapeDtypeStruct((SEQ, 1024), BF16),
            jax.ShapeDtypeStruct((SEQ, 1024), BF16),
            jax.ShapeDtypeStruct((64, 128), F32),
        ),
        in_specs=[anywhere] * 6 + [vmem] * 2,
        out_specs=(vmem, vmem, vmem),
        scratch_shapes=[
            pltpu.VMEM((2, NZ, 8, D), BF16),
            pltpu.VMEM((PROMPT, D), BF16),
            pltpu.VMEM((64, D), BF16),
            pltpu.VMEM((SEQ, D), BF16),
            pltpu.VMEM((SEQ, 1024), BF16),
            pltpu.VMEM((SEQ, 1024), BF16),
            pltpu.VMEM((SEQ, D), BF16),
            pltpu.VMEM((KV_HEADS, HEAD, 512), BF16),
            pltpu.VMEM((KV_HEADS, HEAD, 512), BF16),
            pltpu.VMEM((KV_HEADS, HEAD, SEQ), BF16),
            pltpu.VMEM((KV_HEADS, HEAD, SEQ), BF16),
            pltpu.VMEM((NZ, 2, 64, PROMPT), BF16),
            pltpu.VMEM((512, PROMPT + SEQ), BF16),
            pltpu.VMEM((512, PROMPT + SEQ), BF16),
            pltpu.VMEM((NZ, 2, 64, PROMPT), BF16),
            pltpu.VMEM((NZ, 64, PROMPT), BF16),
            pltpu.VMEM((NZ, 64, PROMPT), BF16),
            pltpu.VMEM((NZ, 64, PROMPT), BF16),
            pltpu.VMEM((NCHIP, 64, 128), F32),
            pltpu.VMEM((NCHIP, 64, 128), BF16),
            pltpu.VMEM((NCHIP, 64, 128), BF16),
            pltpu.VMEM((NCHIP, 64, 128), BF16),
            pltpu.VMEM((NCHIP, 64, 128), BF16),
            dma((6,)),
            dma((NZ, nslot)), dma((NZ, nslot)), dma((NZ, NCH)), dma((NZ, NCH)),
            dma((NZ, 2)), dma((NZ, 2)), dma((NZ, 2)), dma((NZ, 2)),
            dma((NZ, 2)), dma((NZ, 2)), dma((NZ,)), dma((NZ,)),
            dma((4,)), dma((4,)), dma((NCHIP,)), dma((NCHIP,)),
        ],
        compiler_params=pltpu.CompilerParams(
            collective_id=0, has_side_effects=True, vmem_limit_bytes=63 * 1024 * 1024
        ),
    )(
        prompt_hidden[0], kv_weight, queries[0], resp_keys[0], resp_values[0], upstream[0],
        signs, lengths,
    )
    return grad_keys[None], grad_values[None], grad_weight


def solution(mesh):
    rows = P("group", "resp", None)
    return jax.shard_map(
        per_device,
        mesh=mesh,
        in_specs=(rows, P("resp", None), rows, rows, rows, rows, P("group", "resp"), P("group", "resp")),
        out_specs=(rows, rows, P("resp", "group")),
        check_vma=False,
    )
```
